16 devices in a mesh: dp: 2 (over y, z), sp: 8 (over x, core).
Axes of the slice: x: 4, y: 2, z: 1, core: 2. Of those that a mesh axis runs over, the one named last changes fastest.
The devices are a block of a 4x4x8 slice.
Arguments:
- x: bfloat16 [8192, 8192], P(('dp', 'sp')), parts along dimension 0
- gain: bfloat16 [8192], replicated
- wq: bfloat16 [8192, 8192], P('sp')
- wk: bfloat16 [8192, 256], P('sp')
- wv: bfloat16 [8192, 256], P('sp')
- wo: bfloat16 [8192, 8192], P('sp')
Outputs:
- output: bfloat16 [8192, 8192], P(('dp', 'sp')), parts along dimension 0
There are 2 independent parts. The reference program is written for one: setup_inputs(seed, part) draws one part's arguments, and reference() takes and returns one part's arrays. A program takes and returns all parts, laid end to end along the dimension named above; an argument that names none is the same for every part.
All inputs are finite; a program needn't handle non-finite values.
Results may differ from the reference program's by a relative error of at most 0.012.
Values are sent between devices in bfloat16 or wider.
A program may use at most 768 MiB of HBM per device.

```python
import jax
import jax.numpy as jnp
from jax import lax

ROWS = 4096
D = 8192
HEADS = 32
KV_HEADS = 1
HEAD = 256
THETA = 10000


def setup_inputs(seed: int = 0, part: int = 0) -> dict:
    kx, kn, kq, kk, kv, ko = jax.random.split(jax.random.key(seed), 6)

    def weights(key, rows, columns):
        return jax.random.normal(key, (rows, columns), jnp.float32) * rows**-0.5

    drawn = {
        "x": jax.random.normal(jax.random.fold_in(kx, part), (ROWS, D), jnp.float32),
        "gain": 1 + 0.1 * jax.random.normal(kn, (D,), jnp.float32),
        "wq": 2 * weights(kq, D, HEADS * HEAD),
        "wk": 2 * weights(kk, D, KV_HEADS * HEAD),
        "wv": 4 * weights(kv, D, KV_HEADS * HEAD),
        "wo": weights(ko, HEADS * HEAD, D),
    }
    return {k: v.astype(jnp.bfloat16) for k, v in drawn.items()}


def normed(x, gain):
    wide = x.astype(jnp.float32)
    scale = lax.rsqrt(jnp.mean(wide * wide, -1, keepdims=True) + 1e-6)
    return (wide * scale * gain.astype(jnp.float32)).astype(jnp.bfloat16)


def turned(t, place, theta):
    half = t.shape[-1] // 2
    angle = place.astype(jnp.float32)[:, None] * theta ** (-jnp.arange(half, dtype=jnp.float32) / half)
    cos, sin = jnp.cos(angle)[:, None], jnp.sin(angle)[:, None]
    a, b = t[..., :half].astype(jnp.float32), t[..., half:].astype(jnp.float32)
    return jnp.concatenate([a * cos - b * sin, b * cos + a * sin], -1).astype(jnp.bfloat16)


def matmul(a, w):
    return jnp.dot(a, w, preferred_element_type=jnp.float32).astype(jnp.bfloat16)


def einsum(form, a, b):
    return jnp.einsum(form, a.astype(jnp.float32), b.astype(jnp.float32))


def attention(q, k, v):
    scores = einsum("tgsd,ugd->gstu", q, k) * q.shape[-1] ** -0.5
    token = jnp.arange(q.shape[0])
    scores = jnp.where(token[:, None] >= token, scores, -jnp.inf)
    weights = jax.nn.softmax(scores, -1).astype(jnp.bfloat16)
    return einsum("gstu,ugd->tgsd", weights, v).astype(jnp.bfloat16)


def reference(x, gain, wq, wk, wv, wo):
    a, place = normed(x, gain), jnp.arange(ROWS)
    q = turned(matmul(a, wq).reshape(ROWS, HEADS, HEAD), place, THETA).reshape(ROWS, KV_HEADS, -1, HEAD)
    k = turned(matmul(a, wk).reshape(ROWS, KV_HEADS, HEAD), place, THETA)
    v = matmul(a, wv).reshape(ROWS, KV_HEADS, HEAD)
    seen = attention(q, k, v).reshape(ROWS, HEADS * HEAD)
    return (x.astype(jnp.float32) + jnp.dot(seen, wo, preferred_element_type=jnp.float32)).astype(jnp.bfloat16)
```

```python
import functools

import jax
import jax.numpy as jnp
from jax import lax
from jax.experimental import pallas as pl
from jax.experimental.pallas import tpu as pltpu
from jax.sharding import PartitionSpec as P

NEG = -1e30
HIDDEN = 2 * NEG
LOG2E = 1.4426950408889634
HEAD = 256
THETA = 10000
PARTS = 4
NORM = 128
MESH = pl.DeviceIdType.MESH


def _dot(a, b, ca, cb):
    return lax.dot_general(a, b, (((ca,), (cb,)), ((), ())), preferred_element_type=jnp.float32)


def _kernel(size, x_ref, wq_ref, wo_ref, wkv_ref, gain_ref, cq_ref, sq_ref, ck_ref, sk_ref,
            y_ref, xs, a_h, wall, wkvall, kvb, q_h, seen, ybuf,
            w_v, a_v, kv_v, q_v, mix_s, top_s, sa_v, st_v, res_v, ks_v,
            w_ss, w_rs, x_ss, x_rs, k_ss, k_rs, s_ss, s_rs, y_ss, y_rs, lsem, wsem):
    chips = size // 2
    own, model = x_ref.shape
    depth, wide = wq_ref.shape[0], w_v.shape[1]
    thin = wkvall.shape[1]
    bk = own
    g, sp = lax.axis_index("dp"), lax.axis_index("sp")
    x, c = sp // 2, sp % 2
    o = 1 - c
    p = g % 2
    m = 2 * p + c
    mate = g + 1 - 2 * p
    ring = lambda at: lax.rem(at + chips, chips)
    dev = lambda grp, at, core: (grp, ring(at) * 2 + core)
    sib, pair, cross = dev(g, x, o), dev(mate, x, c), dev(mate, x, o)
    shard = lambda at, core: ring(at) * 2 + core
    member = lambda r: (2 * (p if r < 2 else 1 - p)) + (c if r % 2 == 0 else o)
    al = pl.multiple_of

    barrier = pltpu.get_barrier_semaphore()
    friends = [sib, pair, cross, dev(g, x + 1, c), dev(g, x + 1, o), dev(g, x - 1, c), dev(g, x - 1, o), dev(g, x + 2, c)]
    for d in friends:
        pl.semaphore_signal(barrier, inc=1, device_id=d, device_id_type=MESH)
    pl.semaphore_wait(barrier, len(friends))

    def remote(src, dst, ss, rs, to):
        return pltpu.make_async_remote_copy(src_ref=src, dst_ref=dst, send_sem=ss, recv_sem=rs, device_id=to, device_id_type=MESH)

    def hop(k, j, w, first, n, dst):
        rows = lambda s: dst.at[pl.ds(al(s * depth, depth), depth)]
        to = [sib, dev(g, x + 1, c), dev(g, x + 1, o), dev(g, x - 1, c), dev(g, x - 1, o), dev(g, x + 1, c), dev(g, x - 1, c)][j]
        if j < 5:
            at = first(m if j in (1, 3) else member(1))
            src = w.at[:, pl.ds(at, n)]
            out = rows(shard(x, c))
        else:
            src = out = rows(shard(x - 1, c) if j == 5 else shard(x + 1, o))
        return remote(src, out, w_ss.at[k, j], w_rs.at[k, j], to)

    def big(k, j, w=wq_ref):
        return hop(k, j, w, lambda mem: al((mem * PARTS + lax.rem(k, PARTS)) * wide, wide), wide, wall.at[k])

    def small(j):
        return hop(2 * PARTS, j, wkv_ref, lambda mem: al(mem * thin, thin), thin, wkvall)

    def start(k):
        @pl.when(k < PARTS)
        def _():
            for j in range(5):
                big(k, j, wq_ref).start()

        @pl.when(k >= PARTS)
        def _():
            for j in range(5):
                big(k, j, wo_ref).start()

    def relay(copy):
        copy(1).wait_recv()
        copy(5).start()
        copy(4).wait_recv()
        copy(6).start()

    def service(k):
        relay(lambda j: big(k, j))

    others = [shard(x, o), shard(x - 1, c), shard(x - 1, o), shard(x + 1, c), shard(x + 1, o), shard(x + 2, c), shard(x + 2, o)]

    def fill(src, dst):
        for i, s in enumerate(others):
            rows = pl.ds(al(s * depth, depth), depth)
            pltpu.make_async_copy(src.at[rows], dst.at[rows], wsem.at[1 + i]).start()

    def load(k):
        def mine(w):
            return pltpu.make_async_copy(w.at[:, pl.ds(al((m * PARTS + lax.rem(k, PARTS)) * wide, wide), wide)],
                                         w_v.at[pl.ds(al(shard(x, c) * depth, depth), depth)], wsem.at[0])

        @pl.when(k < PARTS)
        def _():
            mine(wq_ref).start()

        @pl.when(k >= PARTS)
        def _():
            mine(wo_ref).start()

        for j in (0, 2, 3, 5, 6):
            big(k, j).wait_recv()
        fill(wall.at[k], w_v)
        mine(wq_ref).wait()
        for i, s in enumerate(others):
            rows = pl.ds(al(s * depth, depth), depth)
            pltpu.make_async_copy(wall.at[k, rows], w_v.at[rows], wsem.at[1 + i]).wait()

    def x_sib():
        return remote(x_ref, xs.at[0, pl.ds(al(c * own, own), own)], x_ss.at[0], x_rs.at[0], sib)

    def x_pair(i):
        return remote(x_ref.at[pl.ds(al(i * NORM, NORM), NORM)], xs.at[1, pl.ds(al(c * own + i * NORM, NORM), NORM)], x_ss.at[1 + i], x_rs.at[1 + i], pair)

    def x_relay(i):
        at = xs.at[1, pl.ds(al(c * own + i * NORM, NORM), NORM)]
        return remote(at, at, x_ss.at[1 + own // NORM + i], x_rs.at[1 + own // NORM + i], sib)

    def norm(src, half, row):
        into = pltpu.make_async_copy(src, a_v.at[0, pl.ds(0, NORM)], lsem.at[0])
        into.start()
        into.wait()

        def some(i, _):
            rows = pl.ds(al(i * 16, 16), 16)
            t = a_v[0, rows, :].astype(jnp.float32)
            scale = lax.rsqrt(jnp.mean(t * t, -1, keepdims=True) + 1e-6)
            a_v[1, rows, :] = (t * scale * gain_ref[...].astype(jnp.float32)).astype(jnp.bfloat16)

        lax.fori_loop(0, NORM // 16, some, None)
        out = pltpu.make_async_copy(a_v.at[1, pl.ds(0, NORM)], a_h.at[half, pl.ds(al(row, NORM), NORM)], lsem.at[1])
        out.start()
        out.wait()

    span = 2 * own
    places = [x, x - 1, x + 1, x + 2]
    at_place = lambda b: pl.ds(al(ring(places[b]) * span, span), span)

    def k_ring(j):
        at = kvb.at[m, :, at_place(0)]
        return remote(at, at, k_ss.at[j], k_rs.at[j], [dev(g, x + 1, c), dev(g, x - 1, c), dev(g, x + 2, c)][j])

    def k_sib(b):
        at = kvb.at[m, :, at_place(b)]
        return remote(at, at, k_ss.at[3 + b], k_rs.at[3 + b], sib)

    def k_pair(b, h):
        return remote(kvb.at[m, h, at_place(b)], kvb.at[m, 1 - h, at_place(b)], k_ss.at[7 + 2 * b + h], k_rs.at[7 + 2 * b + h], pair)

    def k_relay(b):
        at = kvb.at[member(2), :, at_place(b)]
        return remote(at, at, k_ss.at[15 + b], k_rs.at[15 + b], sib)

    def k_forward(b):
        for h in range(2):
            k_pair(b, h).start()
        k_sib(b).start()

    def tile(src, half, row, slot):
        return pltpu.make_async_copy(src.at[half, pl.ds(al(row, own), own)], a_v.at[slot], lsem.at[slot])

    def tiles(src, spot, body):
        def one(u, _):
            slot = lax.rem(u, 2)

            @pl.when(u < 3)
            def _():
                tile(src, *spot(u + 1), 1 - slot).start()

            tile(src, *spot(u), slot).wait()
            body(u, slot)

        lax.fori_loop(0, 4, one, None)

    plain = lambda u: (u // 2, lax.rem(u, 2) * own)

    def keys(u, slot):
        half, row = plain(u)
        t = jnp.dot(a_v[slot], w_v[:, :thin], preferred_element_type=jnp.float32).astype(jnp.bfloat16)
        n = thin // 2
        lo, hi = t[:, :n].astype(jnp.float32), t[:, n:].astype(jnp.float32)
        rows = pl.ds(al(row, own), own)
        cos, sin = ck_ref[rows, :], sk_ref[rows, :]
        ks_v[...] = jnp.concatenate([lo * cos - hi * sin, hi * cos + lo * sin], -1).astype(jnp.bfloat16)
        out = pltpu.make_async_copy(ks_v, kvb.at[m, half, pl.ds(al(x * span + row, own), own)], lsem.at[2])
        out.start()
        out.wait()

    def project(i):
        tile(a_h, *plain(0), 0).start()
        load(i)

        def body(u, slot):
            half, row = plain(u)
            s = jnp.dot(a_v[slot], w_v[...], preferred_element_type=jnp.float32).astype(jnp.bfloat16)
            rows = pl.ds(al(row, own), own)
            cos, sin = cq_ref[rows, :], sq_ref[rows, :]
            low = lax.broadcasted_iota(jnp.int32, cos.shape, 1) < HEAD // 4
            for h in range(wide // HEAD):
                lo = s[:, h * HEAD : h * HEAD + HEAD // 2].astype(jnp.float32)
                hi = s[:, h * HEAD + HEAD // 2 : (h + 1) * HEAD].astype(jnp.float32)
                ta, tb = lo * cos - hi * sin, hi * cos + lo * sin
                st_v[h, :, : HEAD // 2] = jnp.where(low, ta, pltpu.roll(tb, HEAD // 4, 1)).astype(jnp.bfloat16)
                st_v[h, :, HEAD // 2 :] = jnp.where(low, pltpu.roll(ta, HEAD // 4, 1), tb).astype(jnp.bfloat16)
            out = pltpu.make_async_copy(st_v, q_h.at[i, half, :, rows], lsem.at[2])
            out.start()
            out.wait()

        tiles(a_h, plain, body)

    def s_copy(i, j):
        h = j % 2
        cols = lambda mem: pl.ds(al((mem * PARTS + i) * wide, wide), wide)
        if j < 2:
            src, dst, to = seen.at[h, :, cols(m)], seen.at[h, :, cols(m)], sib
        elif j < 4:
            src, dst, to = seen.at[h, :, cols(m)], seen.at[1 - h, :, cols(m)], pair
        else:
            src, dst, to = seen.at[h, :, cols(member(2))], seen.at[h, :, cols(member(2))], sib
        return remote(src, dst, s_ss.at[i, j], s_rs.at[i, j], to)

    def s_relay(i):
        s_copy(i, 2).wait_recv()
        s_copy(i, 3).wait_recv()
        s_copy(i, 4).start()
        s_copy(i, 5).start()

    e = HEAD**-0.5 * LOG2E
    strips = [(h, n, qh) for h in range(2) for n in range(2) for qh in range(2)]
    ones = jnp.ones((8, bk), jnp.bfloat16)

    def attend(i):
        get = pltpu.make_async_copy(q_h.at[i], q_v, lsem.at[2])
        get.start()
        top_s[...] = jnp.full_like(top_s, NEG)
        mix_s[...] = jnp.zeros_like(mix_s)
        get.wait()

        def block(j, which, masked):
            here = pl.ds(al(j * bk, bk), bk)
            cols = lambda t: pl.ds(strips.index(t) * own, own)
            lists = [t for t in strips if t[2] in which]
            ks = [jnp.concatenate([kv_v[0, h, here, :], kv_v[1, h, here, :]], axis=1) for h in range(2)]
            scores = [_dot(ks[h], q_v[h, n, qh * own : (qh + 1) * own, :], 1, 1) for h, n, qh in lists]
            weights, keeps = [], []
            for t, s in zip(lists, scores):
                if t[2] == masked:
                    ok = lax.broadcasted_iota(jnp.int32, s.shape, 1) >= lax.broadcasted_iota(jnp.int32, s.shape, 0)
                    s = jnp.where(ok, s, HIDDEN)
                old = top_s[:, cols(t)]
                top = jnp.maximum(old, s.max(axis=0, keepdims=True))
                top_s[:, cols(t)] = top
                weights.append(jnp.exp2((s - top) * e).astype(jnp.bfloat16))
                keeps.append(jnp.exp2((old - top) * e))
            vs = [jnp.concatenate([kv_v[2, h, here, :].T, kv_v[3, h, here, :].T, ones], axis=0) for h in range(2)]
            for t, w, keep in zip(lists, weights, keeps):
                mix_s[:, cols(t)] = mix_s[:, cols(t)] * keep + _dot(vs[t[0]], w, 1, 0)

        lax.fori_loop(0, 2 * x, lambda j, _: block(j, (0, 1), None), None)
        block(2 * x, (0, 1), 0)
        block(2 * x + 1, (1,), 1)
        for t in strips:
            h, n, qh = t
            here = pl.ds(strips.index(t) * own, own)
            out = mix_s[:HEAD, here] * (1 / mix_s[HEAD : HEAD + 1, here])
            sa_v[h, qh * own : (qh + 1) * own, n * HEAD : (n + 1) * HEAD] = out.T.astype(jnp.bfloat16)
        puts = [pltpu.make_async_copy(sa_v.at[h], seen.at[h, :, pl.ds(al((m * PARTS + i) * wide, wide), wide)], lsem.at[2 + h]) for h in range(2)]
        for put in puts:
            put.start()
        for put in puts:
            put.wait()
        for j in (3, 2, 0, 1):
            s_copy(i, j).start()

    def y_copy(j, u):
        cols = pl.ds(al((m * PARTS + j) * wide, wide), wide)
        return remote(ybuf.at[j, u], y_ref.at[:, cols], y_ss.at[j, u], y_rs.at[j, u], [pair, cross, sib][u])

    def spot(u):
        far = jnp.where(u < 2, 1, 0)
        core = jnp.where((u == 0) | (u == 3), c, o)
        return far, core * own

    def finish(j):
        tile(seen, *spot(0), 0).start()
        load(PARTS + j)
        cols = pl.ds(al((m * PARTS + j) * wide, wide), wide)

        def body(u, slot):
            half, row = spot(u)
            near = pltpu.make_async_copy(x_ref.at[:, cols], res_v, lsem.at[2])
            far = pltpu.make_async_copy(xs.at[half, pl.ds(al(row, own), own), cols], res_v, lsem.at[2])

            @pl.when(u == 3)
            def _():
                near.start()

            @pl.when(u < 3)
            def _():
                far.start()

            s = jnp.dot(a_v[slot], w_v[...], preferred_element_type=jnp.float32)
            near.wait()
            st_v[0] = (res_v[:, : wide // 2].astype(jnp.float32) + s[:, : wide // 2]).astype(jnp.bfloat16)
            st_v[1] = (res_v[:, wide // 2 :].astype(jnp.float32) + s[:, wide // 2 :]).astype(jnp.bfloat16)

            def put(dst):
                n = wide // 2
                moves = [pltpu.make_async_copy(st_v.at[0], dst.at[:, pl.ds(0, n)], lsem.at[2]), pltpu.make_async_copy(st_v.at[1], dst.at[:, pl.ds(n, n)], lsem.at[3])]
                for t in moves:
                    t.start()
                for t in moves:
                    t.wait()

            @pl.when(u == 3)
            def _():
                put(y_ref.at[:, cols])

            for r in range(3):
                @pl.when(u == r)
                def _():
                    put(ybuf.at[j, r])
                    y_copy(j, r).start()

        tiles(seen, spot, body)

    pieces = own // NORM
    for j in range(5):
        small(j).start()
    start(0)
    x_sib().start()
    for i in range(pieces):
        x_pair(i).start()

    lax.fori_loop(0, pieces, lambda i, _: norm(x_ref.at[pl.ds(al(i * NORM, NORM), NORM)], 0, c * own + i * NORM), None)
    relay(small)
    start(1)
    x_sib().wait_recv()
    lax.fori_loop(0, pieces, lambda i, _: norm(xs.at[0, pl.ds(al(o * own + i * NORM, NORM), NORM)], 0, o * own + i * NORM), None)

    def far(i, _):
        x_pair(i).wait_recv()
        x_relay(i).start()
        norm(xs.at[1, pl.ds(al(c * own + i * NORM, NORM), NORM)], 1, c * own + i * NORM)
        x_relay(i).wait_recv()
        norm(xs.at[1, pl.ds(al(o * own + i * NORM, NORM), NORM)], 1, o * own + i * NORM)

        @pl.when(i < 2)
        def _():
            service(i)

        @pl.when(i == 0)
        def _():
            start(2)

    lax.fori_loop(0, pieces, far, None)
    service(2)
    for j in (0, 2, 3, 5, 6):
        small(j).wait_recv()
    tile(a_h, *plain(0), 0).start()
    mine = pltpu.make_async_copy(wkv_ref.at[:, pl.ds(al(m * thin, thin), thin)], w_v.at[pl.ds(al(shard(x, c) * depth, depth), depth), pl.ds(0, thin)], wsem.at[0])
    mine.start()
    fill(wkvall, w_v.at[:, pl.ds(0, thin)])
    mine.wait()
    for i, s in enumerate(others):
        rows = pl.ds(al(s * depth, depth), depth)
        pltpu.make_async_copy(wkvall.at[rows], w_v.at[rows, pl.ds(0, thin)], wsem.at[1 + i]).wait()
    tiles(a_h, plain, keys)
    for j in range(3):
        k_ring(j).start()
    k_forward(0)
    start(3)

    def middle(s, _):
        attends = (s == 3) | (s > 4)
        query = jnp.where(s > 3, 3, s)
        part = jnp.where(s > 4, s - 4, 0)

        @pl.when(s == 1)
        def _():
            for b in range(1, 4):
                k_ring(b - 1).wait_recv()
                k_forward(b)

        @pl.when(s == 3)
        def _():
            for b in range(4):
                for h in range(2):
                    k_pair(b, h).wait_recv()
                k_relay(b).start()
            service(3)
            start(4)
            start(5)
            for b in range(4):
                k_sib(b).wait_recv()
                k_relay(b).wait_recv()
            get = pltpu.make_async_copy(kvb, kv_v, lsem.at[2])
            get.start()
            get.wait()

        @pl.when(jnp.logical_not(attends))
        def _():
            project(query)

        @pl.when(attends)
        def _():
            attend(part)

        @pl.when(s == 5)
        def _():
            service(4)
            start(6)
            s_relay(0)

        @pl.when(s == 6)
        def _():
            service(5)
            start(7)
            s_relay(1)

    lax.fori_loop(0, 8, middle, None)
    s_relay(2)
    service(6)
    s_relay(3)
    for i in range(PARTS):
        for j in (0, 1, 4, 5):
            s_copy(i, j).wait_recv()

    def last(j, _):
        finish(j)

        @pl.when(j == 0)
        def _():
            service(7)

    lax.fori_loop(0, PARTS, last, None)

    for j in range(PARTS):
        for u in range(3):
            y_copy(j, u).wait()
    for j in range(7):
        small(j).wait_send()

    def gone(k, _):
        for j in range(7):
            big(k, j).wait_send()

    lax.fori_loop(0, 2 * PARTS, gone, None)
    x_sib().wait_send()
    for i in range(pieces):
        x_pair(i).wait_send()
        x_relay(i).wait_send()
    for j in range(3):
        k_ring(j).wait_send()
    for b in range(4):
        k_sib(b).wait_send()
        k_relay(b).wait_send()
        for h in range(2):
            k_pair(b, h).wait_send()

    def left(i, _):
        for j in range(6):
            s_copy(i, j).wait_send()

    lax.fori_loop(0, PARTS, left, None)


def angles(place, half, theta):
    angle = place.astype(jnp.float32)[:, None] * theta ** (-jnp.arange(half, dtype=jnp.float32) / half)
    return jnp.cos(angle), jnp.sin(angle)


def solution(mesh):
    size = mesh.shape["sp"]
    chips = size // 2

    def step(x, gain, wq, wk, wv, wo):
        own, model = x.shape
        depth, wide = wq.shape[0], wq.shape[1] // 4 // PARTS
        deep, span = depth * size, 2 * own
        sp, dp = lax.axis_index("sp"), lax.axis_index("dp")
        n = HEAD // 4
        wkv = jnp.concatenate([wk[:, :n], wk[:, 2 * n : 3 * n], wk[:, n : 2 * n], wk[:, 3 * n :], wv], 1)
        cos, sin = angles((sp // 2) * span + jnp.arange(span), HEAD // 2, THETA)
        c, values = sp % 2 == 0, dp % 2 == 1
        ck = jnp.where(values, 1.0, jnp.where(c, cos[:, :n], cos[:, n:]))
        sk = jnp.where(values, 0.0, jnp.where(c, sin[:, :n], sin[:, n:]))
        any_, vmem = pl.BlockSpec(memory_space=pl.ANY), pl.BlockSpec(memory_space=pltpu.VMEM)
        bf = lambda *shape: jax.ShapeDtypeStruct(shape, jnp.bfloat16)
        dma = pltpu.SemaphoreType.DMA
        v = lambda *shape: pltpu.VMEM(shape, jnp.bfloat16)
        outs = pl.pallas_call(
            functools.partial(_kernel, size),
            in_specs=[any_] * 4 + [vmem] * 5,
            out_specs=[any_] * 9,
            out_shape=[bf(own, model), bf(2, span, model), bf(2, span, model), bf(2 * PARTS, deep, wide), bf(deep, HEAD // 2), bf(4, 2, chips * span, HEAD // 2),
                       bf(PARTS, 2, wide // HEAD, span, HEAD), bf(2, span, model), bf(PARTS, 3, own, wide)],
            scratch_shapes=[v(deep, wide), v(2, own, model), v(4, 2, chips * span, HEAD // 2), v(2, wide // HEAD, span, HEAD),
                            pltpu.VMEM((HEAD + 8, 8 * own), jnp.float32), pltpu.VMEM((1, 8 * own), jnp.float32),
                            v(2, span, wide), v(2, own, wide // 2), v(own, wide), v(own, HEAD // 2),
                            dma((2 * PARTS + 1, 7)), dma((2 * PARTS + 1, 7)), dma((9,)), dma((9,)), dma((19,)), dma((19,)),
                            dma((PARTS, 6)), dma((PARTS, 6)), dma((PARTS, 3)), dma((PARTS, 3)), dma((4,)), dma((8,))],
            compiler_params=pltpu.CompilerParams(collective_id=0, has_side_effects=True, vmem_limit_bytes=67043328),
        )(x, wq, wo, wkv, gain[None], cos, sin, ck, sk)
        return outs[0]

    tokens, whole = P(("dp", "sp"), None), P("sp", None)
    return jax.shard_map(
        step,
        mesh=mesh,
        in_specs=(tokens, P(None), whole, whole, whole, whole),
        out_specs=tokens,
        check_vma=False,
    )
```

```python
import functools

import jax
import jax.numpy as jnp
from jax import lax
from jax.experimental import pallas as pl
from jax.experimental.pallas import tpu as pltpu
from jax.sharding import PartitionSpec as P

NEG = -1e30
HIDDEN = 2 * NEG
LOG2E = 1.4426950408889634
HEAD = 256
THETA = 10000
PARTS = 4
TAIL = 2
NORM = 128
MESH = pl.DeviceIdType.MESH


def _dot(a, b, ca, cb):
    return lax.dot_general(a, b, (((ca,), (cb,)), ((), ())), preferred_element_type=jnp.float32)


def _kernel(size, x_ref, wq_ref, wo_ref, wk_ref, wv_ref, gain_ref, cq_ref, sq_ref,
            y_ref, xs, a_h, wall, wkvall, kraw, kother, kvb, q_h, seen, ybuf,
            w_v, a_v, kv_v, q_v, mix_s, top_s, sa_v, st_v, res_v, ks_v, acc_v,
            w_ss, w_rs, x_ss, x_rs, k_ss, k_rs, s_ss, s_rs, y_ss, y_rs, r_ss, r_rs, z_ss, z_rs, lsem, wsem):
    chips = size // 2
    own, model = x_ref.shape
    depth, wide = wq_ref.shape[0], w_v.shape[1]
    thin = wkvall.shape[1]
    bk = own
    g, sp = lax.axis_index("dp"), lax.axis_index("sp")
    x, c = sp // 2, sp % 2
    o = 1 - c
    p = g % 2
    m = 2 * p + c
    mate = g + 1 - 2 * p
    ring = lambda at: lax.rem(at + chips, chips)
    dev = lambda grp, at, core: (grp, ring(at) * 2 + core)
    sib, pair, cross = dev(g, x, o), dev(mate, x, c), dev(mate, x, o)
    shard = lambda at, core: ring(at) * 2 + core
    member = lambda r: (2 * (p if r < 2 else 1 - p)) + (c if r % 2 == 0 else o)
    al = pl.multiple_of

    barrier = pltpu.get_barrier_semaphore()
    friends = [sib, pair, cross, dev(g, x + 1, c), dev(g, x + 1, o), dev(g, x - 1, c), dev(g, x - 1, o)]
    for d in friends:
        pl.semaphore_signal(barrier, inc=1, device_id=d, device_id_type=MESH)
    pl.semaphore_wait(barrier, len(friends))

    def remote(src, dst, ss, rs, to):
        return pltpu.make_async_remote_copy(src_ref=src, dst_ref=dst, send_sem=ss, recv_sem=rs, device_id=to, device_id_type=MESH)

    def hop(k, j, w, first, n, dst):
        rows = lambda s: dst.at[pl.ds(al(s * depth, depth), depth)]
        to = [sib, dev(g, x + 1, c), dev(g, x + 1, o), dev(g, x - 1, c), dev(g, x - 1, o), dev(g, x + 1, c), dev(g, x - 1, c)][j]
        if j < 5:
            at = first(m if j in (1, 3) else member(1))
            src = w.at[:, pl.ds(at, n)]
            out = rows(shard(x, c))
        else:
            src = out = rows(shard(x - 1, c) if j == 5 else shard(x + 1, o))
        return remote(src, out, w_ss.at[k, j], w_rs.at[k, j], to)

    def big(k, j, w=wq_ref):
        return hop(k, j, w, lambda mem: al((mem * PARTS + lax.rem(k, PARTS)) * wide, wide), wide, wall.at[k])

    def small(j, w=wk_ref):
        return hop(2 * PARTS, j, w, lambda mem: al(lax.rem(mem, 2) * thin, thin), thin, wkvall)

    def of_pair(do):
        for n, w in enumerate((wk_ref, wv_ref)):
            @pl.when(p == n)
            def _():
                do(w)

    def start(k, which=range(5)):
        for j in which:
            big(k, j, wq_ref if k < PARTS else wo_ref).start()

    def relay(copy):
        copy(1).wait_recv()
        copy(5).start()
        copy(4).wait_recv()
        copy(6).start()

    def service(k):
        relay(lambda j: big(k, j))

    tail = r_ss.shape[0]
    strip = wide // tail

    def last_hop(n, j):
        at = wall.at[2 * PARTS - 1, pl.ds(al((shard(x + 1, o) if j else shard(x - 1, c)) * depth, depth), depth), pl.ds(al(n * strip, strip), strip)]
        return remote(at, at, r_ss.at[n, j], r_rs.at[n, j], dev(g, x - 1, c) if j else dev(g, x + 1, c))

    def last_service():
        big(2 * PARTS - 1, 1).wait_recv()
        for n in range(tail):
            last_hop(n, 0).start()
        big(2 * PARTS - 1, 4).wait_recv()
        for n in range(tail):
            last_hop(n, 1).start()

    others = [shard(x, o), shard(x - 1, c), shard(x - 1, o), shard(x + 1, c), shard(x + 1, o), shard(x + 2, c), shard(x + 2, o)]

    def fill(src, dst):
        for i, s in enumerate(others):
            rows = pl.ds(al(s * depth, depth), depth)
            pltpu.make_async_copy(src.at[rows], dst.at[rows], wsem.at[1 + i]).start()

    def load(k):
        def mine(w):
            return pltpu.make_async_copy(w.at[:, pl.ds(al((m * PARTS + lax.rem(k, PARTS)) * wide, wide), wide)],
                                         w_v.at[pl.ds(al(shard(x, c) * depth, depth), depth)], wsem.at[0])

        @pl.when(k < PARTS)
        def _():
            mine(wq_ref).start()

        @pl.when(k >= PARTS)
        def _():
            mine(wo_ref).start()

        for j in (0, 2, 3, 5, 6):
            big(k, j).wait_recv()
        fill(wall.at[k], w_v)
        mine(wq_ref).wait()
        for i, s in enumerate(others):
            rows = pl.ds(al(s * depth, depth), depth)
            pltpu.make_async_copy(wall.at[k, rows], w_v.at[rows], wsem.at[1 + i]).wait()

    def x_sib():
        return remote(x_ref, xs.at[0, pl.ds(al(c * own, own), own)], x_ss.at[0], x_rs.at[0], sib)

    def x_pair(i):
        return remote(x_ref.at[pl.ds(al(i * NORM, NORM), NORM)], xs.at[1, pl.ds(al(c * own + i * NORM, NORM), NORM)], x_ss.at[1 + i], x_rs.at[1 + i], pair)

    def x_relay(i):
        at = xs.at[1, pl.ds(al(c * own + i * NORM, NORM), NORM)]
        return remote(at, at, x_ss.at[1 + own // NORM + i], x_rs.at[1 + own // NORM + i], sib)

    def norm(src, half, row):
        into = pltpu.make_async_copy(src, a_v.at[0, pl.ds(0, NORM)], lsem.at[0])
        into.start()
        into.wait()

        def some(i, _):
            rows = pl.ds(al(i * 16, 16), 16)
            t = a_v[0, rows, :].astype(jnp.float32)
            scale = lax.rsqrt(jnp.mean(t * t, -1, keepdims=True) + 1e-6)
            a_v[1, rows, :] = (t * scale * gain_ref[...].astype(jnp.float32)).astype(jnp.bfloat16)

        lax.fori_loop(0, NORM // 16, some, None)
        rows = pl.ds(al(row, NORM), NORM)
        out = pltpu.make_async_copy(a_v.at[1, pl.ds(0, NORM)], a_h.at[half, rows], lsem.at[1])
        out.start()
        ks_v[...] = jnp.dot(a_v[1, :NORM, :], w_v[:, :thin], preferred_element_type=jnp.float32).astype(jnp.bfloat16)
        raw = pltpu.make_async_copy(ks_v, kraw.at[half, rows], lsem.at[2])
        raw.start()
        out.wait()
        raw.wait()

    span = 2 * own
    places = [x, x - 1, x + 1, x + 2]
    at_place = lambda b: pl.ds(al(ring(places[b]) * span, span), span)

    def k_ring(h, j):
        at = kvb.at[m, h, at_place(0)]
        return remote(at, at, k_ss.at[h, j], k_rs.at[h, j], [dev(g, x + 1, c), dev(g, x - 1, c)][j])

    def k_on(h, j):
        at = kvb.at[m, h, pl.ds(al(ring(places[1 + j]) * span + j * own, own), own)]
        return remote(at, at, k_ss.at[h, 2 + j], k_rs.at[h, 2 + j], [dev(g, x + 1, c), dev(g, x - 1, c)][j])

    def k_swap(h):
        return remote(kraw.at[h], kother.at[h], k_ss.at[h, 4], k_rs.at[h, 4], sib)

    def k_sib(h, b):
        at = kvb.at[m, h, at_place(b)]
        return remote(at, at, k_ss.at[h, 5 + b], k_rs.at[h, 5 + b], sib)

    def k_pair(h, b):
        return remote(kvb.at[m, h, at_place(b)], kvb.at[m, 1 - h, at_place(b)], k_ss.at[h, 9 + b], k_rs.at[h, 9 + b], pair)

    def k_relay(h, b):
        at = kvb.at[member(2), h, at_place(b)]
        return remote(at, at, k_ss.at[h, 13 + b], k_rs.at[h, 13 + b], sib)

    def k_forward(h, b):
        k_pair(h, b).start()
        k_sib(h, b).start()

    def tile(src, half, row, slot):
        return pltpu.make_async_copy(src.at[half, pl.ds(al(row, own), own)], a_v.at[slot], lsem.at[slot])

    def tiles(src, spot, body):
        def one(u, _):
            slot = lax.rem(u, 2)

            @pl.when(u < 3)
            def _():
                tile(src, *spot(u + 1), 1 - slot).start()

            tile(src, *spot(u), slot).wait()
            body(u, slot)

        lax.fori_loop(0, 4, one, None)

    plain = lambda u: (u // 2, lax.rem(u, 2) * own)

    def turn_keys(h):
        k_swap(h).start()
        into = pltpu.make_async_copy(kraw.at[h], sa_v.at[0, :, pl.ds(0, thin)], lsem.at[2])
        into.start()
        k_swap(h).wait_recv()
        other = pltpu.make_async_copy(kother.at[h], sa_v.at[0, :, pl.ds(thin, thin)], lsem.at[3])
        other.start()
        into.wait()
        other.wait()
        sign = jnp.where(c == 0, -1.0, 1.0)
        for row in range(0, span, own):
            rows = slice(row, row + own)
            cos, sin = cq_ref[rows, :], sq_ref[rows, :] * sign
            t = sa_v[0, rows, :thin]
            turned = (t.astype(jnp.float32) * cos + sa_v[0, rows, thin : 2 * thin].astype(jnp.float32) * sin).astype(jnp.bfloat16)
            sa_v[0, rows, 2 * thin : 3 * thin] = jnp.where(p == 0, turned, t)
        out = pltpu.make_async_copy(sa_v.at[0, :, pl.ds(2 * thin, thin)], kvb.at[m, h, at_place(0)], lsem.at[2])
        out.start()
        out.wait()
        for j in range(2):
            k_ring(h, j).start()
        k_forward(h, 0)

    def pass_keys(h):
        for j in range(2):
            k_ring(h, j).wait_recv()
            k_on(h, j).start()
        k_forward(h, 1)
        k_forward(h, 2)

    def end_keys(h):
        for j in range(2):
            k_on(h, j).wait_recv()
        k_forward(h, 3)

    def project(i):
        tile(a_h, *plain(0), 0).start()
        load(i)

        def body(u, slot):
            half, row = plain(u)
            s = jnp.dot(a_v[slot], w_v[...], preferred_element_type=jnp.float32).astype(jnp.bfloat16)
            rows = pl.ds(al(row, own), own)
            cos, sin = cq_ref[rows, :], sq_ref[rows, :]
            for h in range(wide // HEAD):
                lo = s[:, h * HEAD : h * HEAD + HEAD // 2].astype(jnp.float32)
                hi = s[:, h * HEAD + HEAD // 2 : (h + 1) * HEAD].astype(jnp.float32)
                st_v[h, :, : HEAD // 2] = (lo * cos - hi * sin).astype(jnp.bfloat16)
                st_v[h, :, HEAD // 2 :] = (hi * cos + lo * sin).astype(jnp.bfloat16)
            out = pltpu.make_async_copy(st_v, q_h.at[i, half, :, rows], lsem.at[2])
            out.start()
            out.wait()

        tiles(a_h, plain, body)

    def s_copy(i, j):
        h = j % 2
        cols = lambda mem: pl.ds(al((mem * PARTS + i) * wide, wide), wide)
        if j < 2:
            src, dst, to = seen.at[h, :, cols(m)], seen.at[h, :, cols(m)], sib
        elif j < 4:
            src, dst, to = seen.at[h, :, cols(m)], seen.at[1 - h, :, cols(m)], pair
        else:
            src, dst, to = seen.at[h, :, cols(member(2))], seen.at[h, :, cols(member(2))], sib
        return remote(src, dst, s_ss.at[i, j], s_rs.at[i, j], to)

    def s_relay(i):
        s_copy(i, 2).wait_recv()
        s_copy(i, 3).wait_recv()
        s_copy(i, 4).start()
        s_copy(i, 5).start()

    e = HEAD**-0.5 * LOG2E
    strips = [(h, n, qh) for h in range(2) for n in range(2) for qh in range(2)]
    ones = jnp.ones((8, bk), jnp.bfloat16)

    def attend(i):
        get = pltpu.make_async_copy(q_h.at[i], q_v, lsem.at[2])
        get.start()
        top_s[...] = jnp.full_like(top_s, NEG)
        mix_s[...] = jnp.zeros_like(mix_s)
        get.wait()

        def block(j, which, masked):
            here = pl.ds(al(j * bk, bk), bk)
            cols = lambda t: pl.ds(strips.index(t) * own, own)
            lists = [t for t in strips if t[2] in which]
            ks = [jnp.concatenate([kv_v[0, h, here, :], kv_v[1, h, here, :]], axis=1) for h in range(2)]
            scores = [_dot(ks[h], q_v[h, n, qh * own : (qh + 1) * own, :], 1, 1) for h, n, qh in lists]
            weights, keeps = [], []
            for t, s in zip(lists, scores):
                if t[2] == masked:
                    ok = lax.broadcasted_iota(jnp.int32, s.shape, 1) >= lax.broadcasted_iota(jnp.int32, s.shape, 0)
                    s = jnp.where(ok, s, HIDDEN)
                old = top_s[:, cols(t)]
                top = jnp.maximum(old, s.max(axis=0, keepdims=True))
                top_s[:, cols(t)] = top
                weights.append(jnp.exp2((s - top) * e).astype(jnp.bfloat16))
                keeps.append(jnp.exp2((old - top) * e))
            vs = [jnp.concatenate([kv_v[2, h, here, :].T, kv_v[3, h, here, :].T, ones], axis=0) for h in range(2)]
            for t, w, keep in zip(lists, weights, keeps):
                mix_s[:, cols(t)] = mix_s[:, cols(t)] * keep + _dot(vs[t[0]], w, 1, 0)

        lax.fori_loop(0, 2 * x, lambda j, _: block(j, (0, 1), None), None)
        block(2 * x, (0, 1), 0)
        block(2 * x + 1, (1,), 1)
        for t in strips:
            h, n, qh = t
            here = pl.ds(strips.index(t) * own, own)
            out = mix_s[:HEAD, here] * (1 / mix_s[HEAD : HEAD + 1, here])
            sa_v[h, qh * own : (qh + 1) * own, n * HEAD : (n + 1) * HEAD] = out.T.astype(jnp.bfloat16)
        puts = [pltpu.make_async_copy(sa_v.at[h], seen.at[h, :, pl.ds(al((m * PARTS + i) * wide, wide), wide)], lsem.at[2 + h]) for h in range(2)]
        for put in puts:
            put.start()
        for put in puts:
            put.wait()
        for j in (3, 2, 0, 1):
            s_copy(i, j).start()

    def y_copy(j, u):
        cols = pl.ds(al((m * PARTS + j) * wide, wide), wide)
        return remote(ybuf.at[j, u], y_ref.at[:, cols], y_ss.at[j, u], y_rs.at[j, u], [pair, cross, sib][u])

    def spot(u):
        far = jnp.where(u < 2, 1, 0)
        core = jnp.where((u == 0) | (u == 3), c, o)
        return far, core * own

    def finish(j):
        tile(seen, *spot(0), 0).start()
        load(PARTS + j)
        cols = pl.ds(al((m * PARTS + j) * wide, wide), wide)

        def body(u, slot):
            half, row = spot(u)
            near = pltpu.make_async_copy(x_ref.at[:, cols], res_v, lsem.at[2])
            far = pltpu.make_async_copy(xs.at[half, pl.ds(al(row, own), own), cols], res_v, lsem.at[2])

            @pl.when(u == 3)
            def _():
                near.start()

            @pl.when(u < 3)
            def _():
                far.start()

            s = jnp.dot(a_v[slot], w_v[...], preferred_element_type=jnp.float32)
            near.wait()
            st_v[0] = (res_v[:, : wide // 2].astype(jnp.float32) + s[:, : wide // 2]).astype(jnp.bfloat16)
            st_v[1] = (res_v[:, wide // 2 :].astype(jnp.float32) + s[:, wide // 2 :]).astype(jnp.bfloat16)

            def put(dst):
                n = wide // 2
                moves = [pltpu.make_async_copy(st_v.at[0], dst.at[:, pl.ds(0, n)], lsem.at[2]), pltpu.make_async_copy(st_v.at[1], dst.at[:, pl.ds(n, n)], lsem.at[3])]
                for t in moves:
                    t.start()
                for t in moves:
                    t.wait()

            @pl.when(u == 3)
            def _():
                put(y_ref.at[:, cols])

            for r in range(3):
                @pl.when(u == r)
                def _():
                    put(ybuf.at[j, r])
                    y_copy(j, r).start()

        tiles(seen, spot, body)

    def z_copy(n, u):
        cols = pl.ds(al((m * PARTS + PARTS - 1) * wide + n * strip, strip), strip)
        return remote(ybuf.at[PARTS - 1, u, :, pl.ds(al(n * strip, strip), strip)], y_ref.at[:, cols], z_ss.at[n, u], z_rs.at[n, u], [pair, cross, sib][u])

    def begin_last():
        k = 2 * PARTS - 1
        tile(seen, *spot(0), 0).start()
        first = (m * PARTS + PARTS - 1) * wide
        mine = pltpu.make_async_copy(wo_ref.at[:, pl.ds(al(first, wide), wide)], w_v.at[pl.ds(al(shard(x, c) * depth, depth), depth)], wsem.at[0])
        mine.start()
        moves = []
        for i, n in enumerate(others[:5]):
            if i in (0, 2, 3):
                big(k, i).wait_recv()
            rows = pl.ds(al(n * depth, depth), depth)
            moves.append(pltpu.make_async_copy(wall.at[k, rows], w_v.at[rows], wsem.at[1 + i]))
            moves[-1].start()
        mine.wait()
        for t in moves:
            t.wait()

        def body(u, slot):
            half, row = spot(u)
            cols = pl.ds(al(first, wide), wide)
            near = pltpu.make_async_copy(x_ref.at[:, cols], res_v, lsem.at[2])
            far = pltpu.make_async_copy(xs.at[half, pl.ds(al(row, own), own), cols], res_v, lsem.at[2])

            @pl.when(u == 3)
            def _():
                near.start()

            @pl.when(u < 3)
            def _():
                far.start()

            total = None
            for at in (x, x - 1, x + 1):
                deep = pl.ds(al(ring(at) * 2 * depth, 2 * depth), 2 * depth)
                t = jnp.dot(a_v[slot, :, deep], w_v[deep, :], preferred_element_type=jnp.float32)
                total = t if total is None else total + t
            near.wait()
            acc_v[u] = res_v[...].astype(jnp.float32) + total

        tiles(seen, spot, body)

    def finish_last():
        k = 2 * PARTS - 1
        first = (m * PARTS + PARTS - 1) * wide
        deep = al(ring(x + 2) * 2 * depth, 2 * depth)
        acts = []
        for u in range(4):
            half, row = spot(u)
            acts.append(pltpu.make_async_copy(seen.at[half, pl.ds(al(row, own), own), pl.ds(deep, 2 * depth)], a_v.at[0, :, pl.ds(u * 2 * depth, 2 * depth)], wsem.at[u]))
            acts[-1].start()
        for t in acts:
            t.wait()

        def some(n, _):
            cols = pl.ds(al(n * strip, strip), strip)
            last_hop(n, 0).wait_recv()
            last_hop(n, 1).wait_recv()
            get = pltpu.make_async_copy(wall.at[k, pl.ds(deep, 2 * depth), cols], w_v.at[pl.ds(0, 2 * depth), pl.ds(0, strip)], wsem.at[0])
            get.start()
            get.wait()
            puts = []
            for u in range(4):
                t = jnp.dot(a_v[0, :, u * 2 * depth : (u + 1) * 2 * depth], w_v[: 2 * depth, :strip], preferred_element_type=jnp.float32)
                sa_v[u // 2, (u % 2) * own : (u % 2 + 1) * own, :strip] = (acc_v[u, :, cols] + t).astype(jnp.bfloat16)
                to = ybuf.at[PARTS - 1, u, :, cols] if u < 3 else y_ref.at[:, pl.ds(al(first + n * strip, strip), strip)]
                puts.append(pltpu.make_async_copy(sa_v.at[u // 2, pl.ds((u % 2) * own, own), pl.ds(0, strip)], to, lsem.at[u]))
                puts[-1].start()
                if u:
                    puts[u - 1].wait()
                    z_copy(n, u - 1).start()
            puts[3].wait()

        lax.fori_loop(0, tail, some, None)

    pieces = own // NORM
    of_pair(lambda w: [small(j, w).start() for j in range(5)])
    x_sib().start()
    for i in range(pieces):
        x_pair(i).start()

    def mine(w):
        return pltpu.make_async_copy(w.at[:, pl.ds(al(c * thin, thin), thin)], w_v.at[pl.ds(al(shard(x, c) * depth, depth), depth), pl.ds(0, thin)], wsem.at[0])

    of_pair(lambda w: mine(w).start())
    relay(small)
    start(0)
    for j in (0, 2, 3, 5, 6):
        small(j).wait_recv()
    fill(wkvall, w_v.at[:, pl.ds(0, thin)])
    mine(wk_ref).wait()
    for i, n in enumerate(others):
        rows = pl.ds(al(n * depth, depth), depth)
        pltpu.make_async_copy(wkvall.at[rows], w_v.at[rows, pl.ds(0, thin)], wsem.at[1 + i]).wait()

    lax.fori_loop(0, pieces, lambda i, _: norm(x_ref.at[pl.ds(al(i * NORM, NORM), NORM)], 0, c * own + i * NORM), None)
    start(1)
    x_sib().wait_recv()
    lax.fori_loop(0, pieces, lambda i, _: norm(xs.at[0, pl.ds(al(o * own + i * NORM, NORM), NORM)], 0, o * own + i * NORM), None)
    turn_keys(0)

    def far(i, _):
        x_pair(i).wait_recv()
        x_relay(i).start()
        norm(xs.at[1, pl.ds(al(c * own + i * NORM, NORM), NORM)], 1, c * own + i * NORM)
        x_relay(i).wait_recv()
        norm(xs.at[1, pl.ds(al(o * own + i * NORM, NORM), NORM)], 1, o * own + i * NORM)

        @pl.when(i < 2)
        def _():
            service(i)

        @pl.when(i == 0)
        def _():
            start(2)

        @pl.when(i == 2)
        def _():
            pass_keys(0)

    lax.fori_loop(0, pieces, far, None)
    turn_keys(1)
    service(2)

    def middle(s, _):
        attends = (s == 2) | (s == 3) | (s == 5) | (s == 7)
        query = jnp.where(s < 2, s, jnp.where(s > 4, 3, 2))
        part = jnp.where(s < 4, jnp.where(s == 3, 1, 0), jnp.where(s > 5, 3, 2))

        @pl.when(s == 1)
        def _():
            pass_keys(1)
            start(3)
            end_keys(0)

        @pl.when(s == 2)
        def _():
            end_keys(1)
            start(4, (0, 1, 3))
            for h in range(2):
                for b in range(4):
                    k_pair(h, b).wait_recv()
                    k_relay(1 - h, b).start()
            for h in range(2):
                for b in range(4):
                    k_sib(h, b).wait_recv()
                    k_relay(h, b).wait_recv()
            get = pltpu.make_async_copy(kvb, kv_v, lsem.at[2])
            get.start()
            get.wait()

        @pl.when(s == 3)
        def _():
            service(3)
            start(4, (2, 4))
            start(5)

        @pl.when(s == 5)
        def _():
            s_relay(0)

        @pl.when(s == 6)
        def _():
            service(4)
            start(6)

        @pl.when(s == 7)
        def _():
            service(5)
            start(7)
            s_relay(1)

        @pl.when(jnp.logical_not(attends))
        def _():
            project(query)

        @pl.when(attends)
        def _():
            attend(part)

    lax.fori_loop(0, 8, middle, None)
    s_relay(2)
    service(6)
    s_relay(3)
    for i in range(PARTS):
        for j in (0, 1, 4, 5):
            s_copy(i, j).wait_recv()

    def most(j, _):
        @pl.when(j == PARTS - 2)
        def _():
            last_service()
            begin_last()

        finish(j)

    lax.fori_loop(0, PARTS - 1, most, None)
    finish_last()

    for n in range(tail):
        for u in range(3):
            z_copy(n, u).wait()
        for j in range(2):
            last_hop(n, j).wait_send()
    for j in range(PARTS - 1):
        for u in range(3):
            y_copy(j, u).wait()
    for j in range(7):
        small(j).wait_send()

    def gone(k, _):
        for j in range(5):
            big(k, j).wait_send()

        @pl.when(k < 2 * PARTS - 1)
        def _():
            for j in (5, 6):
                big(k, j).wait_send()

    lax.fori_loop(0, 2 * PARTS, gone, None)
    x_sib().wait_send()
    for i in range(pieces):
        x_pair(i).wait_send()
        x_relay(i).wait_send()
    for h in range(2):
        k_swap(h).wait_send()
        for j in range(2):
            k_ring(h, j).wait_send()
            k_on(h, j).wait_send()
        for b in range(4):
            k_sib(h, b).wait_send()
            k_relay(h, b).wait_send()
            k_pair(h, b).wait_send()

    def left(i, _):
        for j in range(6):
            s_copy(i, j).wait_send()

    lax.fori_loop(0, PARTS, left, None)


def angles(place, half, theta):
    angle = place.astype(jnp.float32)[:, None] * theta ** (-jnp.arange(half, dtype=jnp.float32) / half)
    return jnp.cos(angle), jnp.sin(angle)


def solution(mesh):
    size = mesh.shape["sp"]
    chips = size // 2

    def step(x, gain, wq, wk, wv, wo):
        own, model = x.shape
        depth, wide = wq.shape[0], wq.shape[1] // 4 // PARTS
        deep, span = depth * size, 2 * own
        cos, sin = angles((lax.axis_index("sp") // 2) * span + jnp.arange(span), HEAD // 2, THETA)
        any_, vmem = pl.BlockSpec(memory_space=pl.ANY), pl.BlockSpec(memory_space=pltpu.VMEM)
        bf = lambda *shape: jax.ShapeDtypeStruct(shape, jnp.bfloat16)
        dma = pltpu.SemaphoreType.DMA
        v = lambda *shape: pltpu.VMEM(shape, jnp.bfloat16)
        outs = pl.pallas_call(
            functools.partial(_kernel, size),
            in_specs=[any_] * 5 + [vmem] * 3,
            out_specs=[any_] * 11,
            out_shape=[bf(own, model), bf(2, span, model), bf(2, span, model), bf(2 * PARTS, deep, wide), bf(deep, HEAD // 2), bf(2, span, HEAD // 2),
                       bf(2, span, HEAD // 2), bf(4, 2, chips * span, HEAD // 2), bf(PARTS, 2, wide // HEAD, span, HEAD), bf(2, span, model), bf(PARTS, 3, own, wide)],
            scratch_shapes=[v(deep, wide), v(2, own, model), v(4, 2, chips * span, HEAD // 2), v(2, wide // HEAD, span, HEAD),
                            pltpu.VMEM((HEAD + 8, 8 * own), jnp.float32), pltpu.VMEM((1, 8 * own), jnp.float32),
                            v(2, span, wide), v(2, own, wide // 2), v(own, wide), v(NORM, HEAD // 2), pltpu.VMEM((4, own, wide), jnp.float32),
                            dma((2 * PARTS + 1, 7)), dma((2 * PARTS + 1, 7)), dma((9,)), dma((9,)), dma((2, 17)), dma((2, 17)),
                            dma((PARTS, 6)), dma((PARTS, 6)), dma((PARTS, 3)), dma((PARTS, 3)), dma((TAIL, 2)), dma((TAIL, 2)), dma((TAIL, 3)), dma((TAIL, 3)),
                            dma((4,)), dma((8,))],
            compiler_params=pltpu.CompilerParams(collective_id=0, has_side_effects=True, vmem_limit_bytes=67043328),
        )(x, wq, wo, wk, wv, gain[None], cos, sin)
        return outs[0]

    tokens, whole = P(("dp", "sp"), None), P("sp", None)
    return jax.shard_map(
        step,
        mesh=mesh,
        in_specs=(tokens, P(None), whole, whole, whole, whole),
        out_specs=tokens,
        check_vma=False,
    )
```

```python
import functools

import jax
import jax.numpy as jnp
from jax import lax
from jax.experimental import pallas as pl
from jax.experimental.pallas import tpu as pltpu
from jax.sharding import PartitionSpec as P

NEG = -1e30
HIDDEN = 2 * NEG
LOG2E = 1.4426950408889634
HEAD = 256
THETA = 10000
PARTS = 4
END, PIECES = PARTS - 1, 2 * PARTS
LAST = PIECES - 1
TAIL = 2
NORM = 128
MESH = pl.DeviceIdType.MESH


def loop(end, body, first=0):
    lax.fori_loop(first, end, lambda i, _: body(i), None)


def run(copies):
    for t in copies:
        t.start()


def local(src, dst, sem):
    return pltpu.make_async_copy(src, dst, sem)


def _dot(a, b, ca, cb):
    return lax.dot_general(a, b, (((ca,), (cb,)), ((), ())), preferred_element_type=jnp.float32)


def _kernel(size, x_ref, wq_ref, wo_ref, wk_ref, wv_ref, gain_ref, freq_ref,
            y_ref, xs, a_h, wall, wkvall, kraw, kother, kvb, q_h, seen, ybuf,
            w_v, a_v, kv_v, q_v, mix_s, top_s, sa_v, st_v, res_v, ks_v, acc_v, wkv_v, cq_ref, sq_ref,
            w_ss, w_rs, x_ss, x_rs, k_ss, k_rs, s_ss, s_rs, y_ss, y_rs, r_ss, r_rs, z_ss, z_rs, lsem, wsem, asem):
    chips = size // 2
    own, model = x_ref.shape
    depth, wide = wq_ref.shape[0], w_v.shape[1]
    thin = wkvall.shape[1]
    bk = own
    g, sp = lax.axis_index("dp"), lax.axis_index("sp")
    x, c = sp // 2, sp % 2
    o = 1 - c
    p = g % 2
    m = 2 * p + c
    mate = g + 1 - 2 * p
    ring = lambda at: lax.rem(at + chips, chips)
    dev = lambda grp, at, core: (grp, ring(at) * 2 + core)
    sib, pair, cross = dev(g, x, o), dev(mate, x, c), dev(mate, x, o)
    shard = lambda at, core: ring(at) * 2 + core
    member = lambda r: (2 * (p if r < 2 else 1 - p)) + (c if r % 2 == 0 else o)
    al = pl.multiple_of

    barrier = pltpu.get_barrier_semaphore()
    friends = [sib, pair, cross, dev(g, x + 1, c), dev(g, x + 1, o), dev(g, x - 1, c), dev(g, x - 1, o)]
    for d in friends:
        pl.semaphore_signal(barrier, inc=1, device_id=d, device_id_type=MESH)
    pl.semaphore_wait(barrier, len(friends))

    def remote(src, dst, ss, rs, to):
        return pltpu.make_async_remote_copy(src_ref=src, dst_ref=dst, send_sem=ss, recv_sem=rs, device_id=to, device_id_type=MESH)

    def hop(k, j, w, first, n, dst):
        rows = lambda s: dst.at[pl.ds(al(s * depth, depth), depth)]
        to = [sib, dev(g, x + 1, c), dev(g, x + 1, o), dev(g, x - 1, c), dev(g, x - 1, o), dev(g, x + 1, c), dev(g, x - 1, c)][j]
        if j < 5:
            at = first(m if j in (1, 3) else member(1))
            src = w.at[:, pl.ds(at, n)]
            out = rows(shard(x, c))
        else:
            src = out = rows(shard(x - 1, c) if j == 5 else shard(x + 1, o))
        return remote(src, out, w_ss.at[k, j], w_rs.at[k, j], to)

    def big(k, j, w=wq_ref):
        return hop(k, j, w, lambda mem: al((mem * PARTS + lax.rem(k, PARTS)) * wide, wide), wide, wall.at[k])

    def small(j, w=wk_ref):
        return hop(PIECES, j, w, lambda mem: al(lax.rem(mem, 2) * thin, thin), thin, wkvall)

    def of_pair(do):
        for n, w in enumerate((wk_ref, wv_ref)):
            @pl.when(p == n)
            def _():
                do(w)

    def start(k, which=range(5)):
        for j in which:
            big(k, j, wq_ref if k < PARTS else wo_ref).start()

    def relay(copy):
        copy(1).wait_recv()
        copy(5).start()
        copy(4).wait_recv()
        copy(6).start()

    def service(k):
        relay(lambda j: big(k, j))

    tail = r_ss.shape[0]
    strip = wide // tail

    def last_hop(n, j):
        at = wall.at[LAST, pl.ds(al((shard(x + 1, o) if j else shard(x - 1, c)) * depth, depth), depth), pl.ds(al(n * strip, strip), strip)]
        return remote(at, at, r_ss.at[n, j], r_rs.at[n, j], dev(g, x - 1, c) if j else dev(g, x + 1, c))

    def last_relay(j):
        big(LAST, 4 if j else 1).wait_recv()
        for n in range(tail):
            last_hop(n, j).start()

    others = [shard(x, o), shard(x - 1, c), shard(x - 1, o), shard(x + 1, c), shard(x + 1, o), shard(x + 2, c), shard(x + 2, o)]

    def fill(src, dst):
        for i, s in enumerate(others):
            rows = pl.ds(al(s * depth, depth), depth)
            local(src.at[rows], dst.at[rows], wsem.at[1 + i]).start()

    def load(k):
        def mine(w):
            return local(w.at[:, pl.ds(al((m * PARTS + lax.rem(k, PARTS)) * wide, wide), wide)],
                                         w_v.at[pl.ds(al(shard(x, c) * depth, depth), depth)], wsem.at[0])

        @pl.when(k < PARTS)
        def _():
            mine(wq_ref).start()

        @pl.when(k >= PARTS)
        def _():
            mine(wo_ref).start()

        for j in (0, 2, 3, 5, 6):
            big(k, j).wait_recv()
        fill(wall.at[k], w_v)
        mine(wq_ref).wait()
        for i, s in enumerate(others):
            rows = pl.ds(al(s * depth, depth), depth)
            local(wall.at[k, rows], w_v.at[rows], wsem.at[1 + i]).wait()

    def x_sib():
        return remote(x_ref, xs.at[0, pl.ds(al(c * own, own), own)], x_ss.at[0], x_rs.at[0], sib)

    def x_pair(i):
        return remote(x_ref.at[pl.ds(al(i * NORM, NORM), NORM)], xs.at[1, pl.ds(al(c * own + i * NORM, NORM), NORM)], x_ss.at[1 + i], x_rs.at[1 + i], pair)

    def x_relay(i):
        at = xs.at[1, pl.ds(al(c * own + i * NORM, NORM), NORM)]
        return remote(at, at, x_ss.at[1 + own // NORM + i], x_rs.at[1 + own // NORM + i], sib)

    def norm(src, half, row):
        into = local(src, a_v.at[0, pl.ds(0, NORM)], lsem.at[0])
        into.start()
        into.wait()

        def some(i):
            rows = pl.ds(al(i * 16, 16), 16)
            t = a_v[0, rows, :].astype(jnp.float32)
            scale = lax.rsqrt(jnp.mean(t * t, -1, keepdims=True) + 1e-6)
            a_v[1, rows, :] = (t * scale * gain_ref[...].astype(jnp.float32)).astype(jnp.bfloat16)

        loop(NORM // 16, some)
        rows = pl.ds(al(row, NORM), NORM)
        out = local(a_v.at[1, pl.ds(0, NORM)], a_h.at[half, rows], lsem.at[1])
        out.start()
        ks_v[...] = jnp.dot(a_v[1, :NORM, :], wkv_v[...], preferred_element_type=jnp.float32).astype(jnp.bfloat16)
        raw = local(ks_v, kraw.at[half, rows], lsem.at[2])
        raw.start()
        out.wait()
        raw.wait()

    span = 2 * own
    places = [x, x - 1, x + 1, x + 2]
    at_place = lambda b: pl.ds(al(ring(places[b]) * span, span), span)

    def k_ring(h, j):
        at = kvb.at[m, h, at_place(0)]
        return remote(at, at, k_ss.at[h, j], k_rs.at[h, j], [dev(g, x + 1, c), dev(g, x - 1, c)][j])

    def k_on(h, j):
        at = kvb.at[m, h, pl.ds(al(ring(places[1 + j]) * span + j * own, own), own)]
        return remote(at, at, k_ss.at[h, 2 + j], k_rs.at[h, 2 + j], [dev(g, x + 1, c), dev(g, x - 1, c)][j])

    def k_swap(h):
        return remote(kraw.at[h], kother.at[h], k_ss.at[h, 4], k_rs.at[h, 4], sib)

    def k_sib(h, b):
        at = kvb.at[m, h, at_place(b)]
        return remote(at, at, k_ss.at[h, 5 + b], k_rs.at[h, 5 + b], sib)

    def k_pair(h, b):
        return remote(kvb.at[m, h, at_place(b)], kvb.at[m, 1 - h, at_place(b)], k_ss.at[h, 9 + b], k_rs.at[h, 9 + b], pair)

    def k_relay(h, b):
        at = kvb.at[member(2), h, at_place(b)]
        return remote(at, at, k_ss.at[h, 13 + b], k_rs.at[h, 13 + b], sib)

    def k_forward(h, b):
        k_pair(h, b).start()
        k_sib(h, b).start()

    def tile(src, half, row, slot):
        return local(src.at[half, pl.ds(al(row, own), own)], a_v.at[slot], lsem.at[slot])

    def tiles(get, body, first=0, end=4):
        def one(u):
            slot = lax.rem(u, 2)

            @pl.when(u + 1 < end)
            def _():
                run(get(u + 1, 1 - slot))

            for t in get(u, slot):
                t.wait()
            body(u, slot)

        loop(end, one, first)

    plain = lambda u: (u // 2, lax.rem(u, 2) * own)

    def turn_keys(h):
        k_swap(h).start()
        into = local(kraw.at[h], sa_v.at[0, :, pl.ds(0, thin)], lsem.at[2])
        into.start()
        k_swap(h).wait_recv()
        other = local(kother.at[h], sa_v.at[0, :, pl.ds(thin, thin)], lsem.at[3])
        other.start()
        into.wait()
        other.wait()
        sign = jnp.where(c == 0, -1.0, 1.0)
        for row in range(0, span, own):
            rows = slice(row, row + own)
            cos, sin = cq_ref[rows, :], sq_ref[rows, :] * sign
            t = sa_v[0, rows, :thin]
            turned = (t.astype(jnp.float32) * cos + sa_v[0, rows, thin : 2 * thin].astype(jnp.float32) * sin).astype(jnp.bfloat16)
            sa_v[0, rows, 2 * thin : 3 * thin] = jnp.where(p == 0, turned, t)
        out = local(sa_v.at[0, :, pl.ds(2 * thin, thin)], kvb.at[m, h, at_place(0)], lsem.at[2])
        out.start()
        out.wait()
        for j in range(2):
            k_ring(h, j).start()
        k_forward(h, 0)

    def pass_keys(h):
        for j in range(2):
            k_ring(h, j).wait_recv()
            k_on(h, j).start()
        k_forward(h, 1)
        k_forward(h, 2)

    def end_keys(h):
        for j in range(2):
            k_on(h, j).wait_recv()
        k_forward(h, 3)

    def project(i, first=0, end=4):
        get = lambda u, slot: [tile(a_h, *plain(u), slot)]
        run(get(first, 0))
        if first == 0:
            load(i)

        def body(u, slot):
            half, row = plain(u)
            s = jnp.dot(a_v[slot], w_v[...], preferred_element_type=jnp.float32).astype(jnp.bfloat16)
            rows = pl.ds(al(row, own), own)
            cos, sin = cq_ref[rows, :], sq_ref[rows, :]
            for h in range(wide // HEAD):
                lo = s[:, h * HEAD : h * HEAD + HEAD // 2].astype(jnp.float32)
                hi = s[:, h * HEAD + HEAD // 2 : (h + 1) * HEAD].astype(jnp.float32)
                st_v[h, :, : HEAD // 2] = (lo * cos - hi * sin).astype(jnp.bfloat16)
                st_v[h, :, HEAD // 2 :] = (hi * cos + lo * sin).astype(jnp.bfloat16)
            out = local(st_v, q_h.at[i, half, :, rows], lsem.at[2])
            out.start()
            out.wait()

        tiles(get, body, first, end)

    def s_copy(i, j):
        h = j % 2
        cols = lambda mem: pl.ds(al((mem * PARTS + i) * wide, wide), wide)
        if j < 2:
            src, dst, to = seen.at[h, :, cols(m)], seen.at[h, :, cols(m)], sib
        elif j < 4:
            src, dst, to = seen.at[h, :, cols(m)], seen.at[1 - h, :, cols(m)], pair
        else:
            src, dst, to = seen.at[h, :, cols(member(2))], seen.at[h, :, cols(member(2))], sib
        return remote(src, dst, s_ss.at[i, j], s_rs.at[i, j], to)

    def s_relay(i):
        s_copy(i, 2).wait_recv()
        s_copy(i, 3).wait_recv()
        s_copy(i, 4).start()
        s_copy(i, 5).start()

    e = HEAD**-0.5 * LOG2E
    strips = [(h, n, qh) for h in range(2) for n in range(2) for qh in range(2)]
    ones = jnp.ones((8, bk), jnp.bfloat16)

    def attend(i):
        get = local(q_h.at[i], q_v, lsem.at[2])
        get.start()
        top_s[...] = jnp.full_like(top_s, NEG)
        mix_s[...] = jnp.zeros_like(mix_s)
        get.wait()

        def block(j, which, masked):
            here = pl.ds(al(j * bk, bk), bk)
            cols = lambda t: pl.ds(strips.index(t) * own, own)
            lists = [t for t in strips if t[2] in which]
            ks = [jnp.concatenate([kv_v[0, h, here, :], kv_v[1, h, here, :]], axis=1) for h in range(2)]
            scores = [_dot(ks[h], q_v[h, n, qh * own : (qh + 1) * own, :], 1, 1) for h, n, qh in lists]
            weights, keeps = [], []
            for t, s in zip(lists, scores):
                if t[2] == masked:
                    ok = lax.broadcasted_iota(jnp.int32, s.shape, 1) >= lax.broadcasted_iota(jnp.int32, s.shape, 0)
                    s = jnp.where(ok, s, HIDDEN)
                old = top_s[:, cols(t)]
                top = jnp.maximum(old, s.max(axis=0, keepdims=True))
                top_s[:, cols(t)] = top
                weights.append(jnp.exp2((s - top) * e).astype(jnp.bfloat16))
                keeps.append(jnp.exp2((old - top) * e))
            vs = [jnp.concatenate([kv_v[2, h, here, :].T, kv_v[3, h, here, :].T, ones], axis=0) for h in range(2)]
            for t, w, keep in zip(lists, weights, keeps):
                mix_s[:, cols(t)] = mix_s[:, cols(t)] * keep + _dot(vs[t[0]], w, 1, 0)

        loop(2 * x, lambda j: block(j, (0, 1), -1))
        block(2 * x, (0, 1), 0)
        block(2 * x + 1, (1,), 1)
        for t in strips:
            h, n, qh = t
            here = pl.ds(strips.index(t) * own, own)
            out = mix_s[:HEAD, here] * (1 / mix_s[HEAD : HEAD + 1, here])
            sa_v[h, qh * own : (qh + 1) * own, n * HEAD : (n + 1) * HEAD] = out.T.astype(jnp.bfloat16)
        puts = [local(sa_v.at[h], seen.at[h, :, pl.ds(al((m * PARTS + i) * wide, wide), wide)], lsem.at[2 + h]) for h in range(2)]
        for put in puts:
            put.start()
        for put in puts:
            put.wait()
        for j in (3, 2, 0, 1):
            s_copy(i, j).start()

    def y_copy(j, u):
        cols = pl.ds(al((m * PARTS + j) * wide, wide), wide)
        return remote(ybuf.at[j, u], y_ref.at[:, cols], y_ss.at[j, u], y_rs.at[j, u], [pair, cross, sib][u])

    def spot(u):
        far = jnp.where(u < 2, 1, 0)
        core = jnp.where((u == 0) | (u == 3), c, o)
        return far, core * own

    def finish(j):
        get = lambda u, slot: [tile(seen, *spot(u), slot)]
        run(get(0, 0))
        load(PARTS + j)
        cols = pl.ds(al((m * PARTS + j) * wide, wide), wide)

        def body(u, slot):
            half, row = spot(u)
            near = local(x_ref.at[:, cols], res_v, lsem.at[2])
            far = local(xs.at[half, pl.ds(al(row, own), own), cols], res_v, lsem.at[2])

            @pl.when(u == 3)
            def _():
                near.start()

            @pl.when(u < 3)
            def _():
                far.start()

            @pl.when((j == PARTS - 2) & (u == 3))
            def _():
                last_relay(1)

            s = jnp.dot(a_v[slot], w_v[...], preferred_element_type=jnp.float32)
            near.wait()
            st_v[0] = (res_v[:, : wide // 2].astype(jnp.float32) + s[:, : wide // 2]).astype(jnp.bfloat16)
            st_v[1] = (res_v[:, wide // 2 :].astype(jnp.float32) + s[:, wide // 2 :]).astype(jnp.bfloat16)

            def put(dst):
                n = wide // 2
                moves = [local(st_v.at[0], dst.at[:, pl.ds(0, n)], lsem.at[2]), local(st_v.at[1], dst.at[:, pl.ds(n, n)], lsem.at[3])]
                for t in moves:
                    t.start()
                for t in moves:
                    t.wait()

            @pl.when(u == 3)
            def _():
                put(y_ref.at[:, cols])

            for r in range(3):
                @pl.when(u == r)
                def _():
                    put(ybuf.at[j, r])
                    y_copy(j, r).start()

        tiles(get, body)

    def z_copy(n, u):
        cols = pl.ds(al((m * PARTS + END) * wide + n * strip, strip), strip)
        return remote(ybuf.at[END, u, :, pl.ds(al(n * strip, strip), strip)], y_ref.at[:, cols], z_ss.at[n, u], z_rs.at[n, u], [pair, cross, sib][u])

    def brought(ranges):
        def get(u, slot):
            half, row = spot(u)
            return [local(seen.at[half, pl.ds(al(row, own), own), r], a_v.at[slot, :, r], asem.at[slot * 4 + i]) for i, r in enumerate(ranges)]

        run(get(0, 0))
        return get

    def begin(j, ranges, get):
        cols = pl.ds(al((m * PARTS + j) * wide, wide), wide)

        def body(u, slot):
            half, row = spot(u)
            near = local(x_ref.at[:, cols], res_v, lsem.at[2])
            far = local(xs.at[half, pl.ds(al(row, own), own), cols], res_v, lsem.at[2])

            @pl.when(u == 3)
            def _():
                near.start()

            @pl.when(u < 3)
            def _():
                far.start()

            total = sum(jnp.dot(a_v[slot, :, r], w_v[r, :], preferred_element_type=jnp.float32) for r in ranges)
            near.wait()
            acc_v[u] = res_v[...].astype(jnp.float32) + total

        tiles(get, body)

    def gather(ranges, put):
        moves = []
        for u in range(4):
            half, row = spot(u)
            for r in ranges:
                moves.append(local(seen.at[half, pl.ds(al(row, own), own), r], put(u, len(moves) % len(ranges)), asem.at[len(moves)]))
                moves[-1].start()
        for t in moves:
            t.wait()

    def settle(j, n, width, add, send):
        cols = pl.ds(al(n * width, width), width)
        puts = []
        for u in range(4):
            half, rows = u // 2, pl.ds(u % 2 * own, own)
            sa_v[half, rows, :width] = (acc_v[u, :, cols] + add(u)).astype(jnp.bfloat16)
            to = ybuf.at[j, u, :, cols] if u < 3 else y_ref.at[:, pl.ds(al((m * PARTS + j) * wide + n * width, width), width)]
            puts.append(local(sa_v.at[half, rows, pl.ds(0, width)], to, lsem.at[u]))
            puts[-1].start()
            if u:
                puts[u - 1].wait()
                send(u - 1).start()
        puts[3].wait()

    shards = lambda s, n=1: pl.ds(al(s * depth, depth), n * depth)

    def begin_last():
        k = LAST
        ranges = [shards(shard(x, 0), 2), shards(shard(x - 1, c)), shards(shard(x + 1, c))]
        get = brought(ranges)
        moves = [local(wo_ref.at[:, pl.ds(al((m * PARTS + END) * wide, wide), wide)], w_v.at[shards(shard(x, c))], wsem.at[0])]
        big(k, 0).wait_recv()
        last_relay(0)
        big(k, 3).wait_recv()
        for i, n in enumerate((shard(x, o), shard(x - 1, c), shard(x + 1, c))):
            moves.append(local(wall.at[k, shards(n)], w_v.at[shards(n)], wsem.at[1 + i]))
        for t in moves:
            t.start()
        for t in moves:
            t.wait()
        begin(END, ranges, get)

    def finish_last():
        k = LAST
        rest = [shards(shard(x - 1, o)), shards(shard(x + 1, o)), shards(shard(x + 2, 0), 2)]
        big(k, 2).wait_recv()
        moves = [local(wall.at[k, r], w_v.at[r], wsem.at[i]) for i, r in enumerate(rest[:2])]
        for t in moves:
            t.start()
        at = lambda u, i: (u % 2 * 4 + i) * depth
        gather(rest, lambda u, i: a_v.at[u // 2, :, pl.ds(at(u, i), rest[i].size)])
        for t in moves:
            t.wait()

        def some(n):
            cols = pl.ds(al(n * strip, strip), strip)
            for j in range(2):
                last_hop(n, j).wait_recv()
            get = local(wall.at[k, rest[2], cols], w_v.at[rest[2], cols], wsem.at[0])
            get.start()
            get.wait()
            add = lambda u: sum(jnp.dot(a_v[u // 2, :, at(u, i) : at(u, i) + r.size], w_v[r, cols], preferred_element_type=jnp.float32) for i, r in enumerate(rest))
            settle(END, n, strip, add, lambda u: z_copy(n, u))

        loop(tail, some)

    pieces = own // NORM
    of_pair(lambda w: [small(j, w).start() for j in range(5)])
    start(0, (0, 1, 3))
    x_sib().start()
    for i in range(pieces):
        x_pair(i).start()

    def mine(w):
        return local(w.at[:, pl.ds(al(c * thin, thin), thin)], wkv_v.at[pl.ds(al(shard(x, c) * depth, depth), depth)], wsem.at[0])

    of_pair(lambda w: mine(w).start())

    def angles(i):
        rows = pl.ds(al(i * NORM, NORM), NORM)
        place = lax.broadcasted_iota(jnp.int32, (NORM, thin), 0) + (x * span + i * NORM)
        angle = place.astype(jnp.float32) * freq_ref[...]
        cq_ref[rows, :], sq_ref[rows, :] = jnp.cos(angle), jnp.sin(angle)

    loop(span // NORM, angles)
    relay(small)
    start(0, (2, 4))
    for j in (0, 2, 3, 5, 6):
        small(j).wait_recv()
    fill(wkvall, wkv_v)
    mine(wk_ref).wait()
    for i, n in enumerate(others):
        rows = pl.ds(al(n * depth, depth), depth)
        local(wkvall.at[rows], wkv_v.at[rows], wsem.at[1 + i]).wait()

    loop(pieces, lambda i: norm(x_ref.at[pl.ds(al(i * NORM, NORM), NORM)], 0, c * own + i * NORM))
    start(1)
    x_sib().wait_recv()
    loop(pieces, lambda i: norm(xs.at[0, pl.ds(al(o * own + i * NORM, NORM), NORM)], 0, o * own + i * NORM))
    turn_keys(0)

    def far(i):
        x_pair(i).wait_recv()
        x_relay(i).start()
        norm(xs.at[1, pl.ds(al(c * own + i * NORM, NORM), NORM)], 1, c * own + i * NORM)
        x_relay(i).wait_recv()
        norm(xs.at[1, pl.ds(al(o * own + i * NORM, NORM), NORM)], 1, o * own + i * NORM)

        @pl.when(i < 2)
        def _():
            service(i)

        @pl.when(i == 0)
        def _():
            start(2)

        @pl.when(i == 2)
        def _():
            pass_keys(0)
            project(0, 0, 2)

    loop(pieces, far)
    turn_keys(1)
    service(2)
    project(0, 2)

    def middle(s):
        attends = (s == 2) | (s == 3) | (s == 5) | (s == 7)
        query = jnp.where(s < 2, s, jnp.where(s > 4, 3, 2))
        part = jnp.where(s < 4, jnp.where(s == 3, 1, 0), jnp.where(s > 5, 3, 2))

        @pl.when(s == 1)
        def _():
            pass_keys(1)
            start(3)
            end_keys(0)

        @pl.when(s == 2)
        def _():
            end_keys(1)
            start(4, (0, 1, 3))
            for h in range(2):
                for b in range(4):
                    k_pair(h, b).wait_recv()
                    k_relay(1 - h, b).start()
            for h in range(2):
                for b in range(4):
                    k_sib(h, b).wait_recv()
                    k_relay(h, b).wait_recv()
            get = local(kvb, kv_v, lsem.at[2])
            get.start()
            get.wait()

        @pl.when(s == 3)
        def _():
            service(3)
            start(4, (2, 4))
            start(5)

        @pl.when(s == 5)
        def _():
            s_relay(0)

        @pl.when(s == 6)
        def _():
            service(4)
            start(6)

        @pl.when(s == 7)
        def _():
            service(5)
            start(7, (0, 1, 3))
            s_relay(1)

        @pl.when(jnp.logical_not(attends))
        def _():
            project(query)

        @pl.when(attends)
        def _():
            attend(part)

    loop(8, middle, 1)
    s_relay(2)
    early, late = range(END), range(END, PARTS)

    def arrived(parts):
        for i in parts:
            for j in (0, 1, 4, 5):
                s_copy(i, j).wait_recv()

    def depths(parts):
        n = len(parts) * wide
        return [pl.ds((mem * PARTS + parts[0]) * wide, n) for mem in range(4)]

    arrived(early)
    get = brought(depths(early))
    load(PARTS)
    begin(0, depths(early), get)
    service(6)
    start(7, (2, 4))
    s_relay(3)
    arrived(late)
    gather(depths(late), lambda u, i: a_v.at[0, :, pl.ds((u * 4 + i) * wide, wide)])
    settle(0, 0, wide, lambda u: sum(jnp.dot(a_v[0, :, (u * 4 + i) * wide : (u * 4 + i + 1) * wide], w_v[r, :], preferred_element_type=jnp.float32)
                                     for i, r in enumerate(depths(late))), lambda u: y_copy(0, u))

    def most(j):
        @pl.when(j == PARTS - 2)
        def _():
            begin_last()

        finish(j)

    loop(END, most, 1)
    finish_last()

    for n in range(tail):
        for u in range(3):
            z_copy(n, u).wait()
        for j in range(2):
            last_hop(n, j).wait_send()
    for j in range(END):
        for u in range(3):
            y_copy(j, u).wait()
    for j in range(7):
        small(j).wait_send()

    def gone(k):
        for j in range(5):
            big(k, j).wait_send()

        @pl.when(k < LAST)
        def _():
            for j in (5, 6):
                big(k, j).wait_send()

    loop(PIECES, gone)
    x_sib().wait_send()
    for i in range(pieces):
        x_pair(i).wait_send()
        x_relay(i).wait_send()
    for h in range(2):
        k_swap(h).wait_send()
        for j in range(2):
            k_ring(h, j).wait_send()
            k_on(h, j).wait_send()
        for b in range(4):
            k_sib(h, b).wait_send()
            k_relay(h, b).wait_send()
            k_pair(h, b).wait_send()

    def left(i):
        for j in range(6):
            s_copy(i, j).wait_send()

    loop(PARTS, left)


def solution(mesh):
    size = mesh.shape["sp"]
    chips = size // 2

    def step(x, gain, wq, wk, wv, wo):
        own, model = x.shape
        depth, wide = wq.shape[0], wq.shape[1] // 4 // PARTS
        deep, span = depth * size, 2 * own
        half = HEAD // 2
        freq = THETA ** (-jnp.arange(half, dtype=jnp.float32) / half)
        any_, vmem = pl.BlockSpec(memory_space=pl.ANY), pl.BlockSpec(memory_space=pltpu.VMEM)
        bf = lambda *shape: jax.ShapeDtypeStruct(shape, jnp.bfloat16)
        dma = pltpu.SemaphoreType.DMA
        v = lambda *shape: pltpu.VMEM(shape, jnp.bfloat16)
        outs = pl.pallas_call(
            functools.partial(_kernel, size),
            in_specs=[any_] * 5 + [vmem] * 2,
            out_specs=[any_] * 11,
            out_shape=[bf(own, model), bf(2, span, model), bf(2, span, model), bf(PIECES, deep, wide), bf(deep, HEAD // 2), bf(2, span, HEAD // 2),
                       bf(2, span, HEAD // 2), bf(4, 2, chips * span, HEAD // 2), bf(PARTS, 2, wide // HEAD, span, HEAD), bf(2, span, model), bf(PARTS, 3, own, wide)],
            scratch_shapes=[v(deep, wide), v(2, own, model), v(4, 2, chips * span, HEAD // 2), v(2, wide // HEAD, span, HEAD),
                            pltpu.VMEM((HEAD + 8, 8 * own), jnp.float32), pltpu.VMEM((1, 8 * own), jnp.float32),
                            v(2, span, wide), v(2, own, wide // 2), v(own, wide), v(NORM, HEAD // 2), pltpu.VMEM((4, own, wide), jnp.float32), v(deep, HEAD // 2), pltpu.VMEM((span, HEAD // 2), jnp.float32), pltpu.VMEM((span, HEAD // 2), jnp.float32),
                            dma((PIECES + 1, 7)), dma((PIECES + 1, 7)), dma((9,)), dma((9,)), dma((2, 17)), dma((2, 17)),
                            dma((PARTS, 6)), dma((PARTS, 6)), dma((PARTS, 3)), dma((PARTS, 3)), dma((TAIL, 2)), dma((TAIL, 2)), dma((TAIL, 3)), dma((TAIL, 3)),
                            dma((4,)), dma((8,)), dma((16,))],
            compiler_params=pltpu.CompilerParams(collective_id=0, has_side_effects=True, vmem_limit_bytes=67043328),
        )(x, wq, wo, wk, wv, gain[None], freq[None])
        return outs[0]

    tokens, whole = P(("dp", "sp"), None), P("sp", None)
    return jax.shard_map(
        step,
        mesh=mesh,
        in_specs=(tokens, P(None), whole, whole, whole, whole),
        out_specs=tokens,
        check_vma=False,
    )
```
